256 devices in a mesh: gx: 32 (over y, z_hi, core), ta: 8 (over x, z_lo).
Axes of the slice: x: 4, y: 4, z: 8 (z_hi: 4, z_lo: 2; z = z_hi * 2 + z_lo), core: 2. Of those that a mesh axis runs over, the one named last changes fastest.
Arguments:
- source: float32 [128, 1024, 512], P('ta', 'gx'), may hold values from -6 to 6
- previous: float32 [128, 1024, 512], P('ta', 'gx'), may hold values from -6 to 6
- time_modes: float32 [128, 128], replicated, as said below
- time_back: float32 [128, 128], replicated, as said below
- step_code: int32 [128], P('ta'), may hold values from 0 to 32
Outputs:
- next_iterate: float32 [128, 1024, 512], P('ta', 'gx')
The draws below stay inside these ranges and needn't reach their ends.
Inputs may be any that keep to these rules, and one draw needn't show every extreme that they name: time_modes times time_back is the identity up to rounding. time_back is the inverse of time_modes up to rounding.
All inputs are finite; a program needn't handle non-finite values.
Results may differ from the reference program's by a relative error of at most 0.0001.
Values sent between devices are 32-bit elements; how exact they have to be, the bound alone decides.
No kernel may reach another device: no remote copies, remote signals or barrier semaphores. Data moves between devices by JAX's collectives and lax.ppermute only.
A program may use at most 64 MiB of HBM per device.

```python
import jax
import jax.numpy as jnp
from jax import lax

CX = 32
CY = 64
CZ = 8
CYCLES = 2
LEVELS = 3
NT = 128
NX = 1024
ZY = 512
N_GX = 32


def time_pair(key):
    noise_key = jax.random.fold_in(key, 7)
    noise = jax.random.normal(noise_key, (NT, NT), jnp.float32)
    back = jnp.eye(NT, dtype=jnp.float32) + 0.3 * noise / jnp.sqrt(NT * 1.0)
    return (back, jnp.linalg.inv(back))


def draw_time_back(key, part):
    return time_pair(key)[0]


def draw_time_modes(key, part):
    return time_pair(key)[1]


def with_ends(entries, key, least, top_value):
    shape = entries.shape
    spot = [jax.random.randint(jax.random.fold_in(key, axis), (), 0, shape[axis]) for axis in range(len(shape))]
    entries = entries.at[tuple(spot)].set(least)
    longest = shape.index(max(shape))
    spot[longest] = (spot[longest] + 1) % shape[longest]
    return entries.at[tuple(spot)].set(top_value)


def block_levels(key, shape, pieces, low, largest):
    def one(dim, shards_of):
        draws = jax.random.uniform(jax.random.fold_in(jax.random.fold_in(key, 6), dim), (shards_of,), jnp.float32, low / len(pieces), largest / len(pieces))
        return jnp.repeat(jnp.exp(draws), shape[dim] // shards_of).reshape((-1,) + (1,) * (len(shape) - dim - 1))

    factor_of = one(*pieces[0])
    for cut in pieces[1:]:
        factor_of = factor_of * one(*cut)
    return factor_of


def normal_values(rng, extent, deviation, limit, shards=(), kind=jnp.bfloat16):
    loudness = block_levels(rng, extent, shards, -0.22, 0.18) if shards else 1.0
    array = jax.random.normal(rng, extent, jnp.float32) * deviation * loudness
    return jnp.minimum(jnp.maximum(array, -limit), limit).astype(kind)


def setup_inputs(seed: int = 0) -> dict:
    arg_keys = jax.random.split(jax.random.key(seed), 6)
    source = normal_values(arg_keys[0], (NT, NX, ZY), 1.0, 6.0, ((0, 8), (1, 32)), jnp.float32)
    previous = normal_values(arg_keys[1], (NT, NX, ZY), 1.0, 6.0, ((0, 8), (1, 32)), jnp.float32)
    time_modes = draw_time_modes(jax.random.fold_in(arg_keys[5], 71), 0)
    time_back = draw_time_back(jax.random.fold_in(arg_keys[5], 71), 0)
    step_code = with_ends(jax.random.randint(arg_keys[4], (NT,), 0, 33), jax.random.fold_in(arg_keys[4], 1), 0, 32).astype(jnp.int32)
    return {"source": source, "previous": previous, "time_modes": time_modes, "time_back": time_back, "step_code": step_code}


ROBIN = 1.0
DAMPING = 0.8

def neighbour_sum(field, zdim, ydim):
    rank = field.ndim
    xpad = jnp.pad(field, [(0, 0)] * (rank - 2) + [(1, 1), (0, 0)])
    total = xpad[..., 2:, :] + xpad[..., :-2, :]
    zpad = jnp.pad(field, [(0, 0)] * (rank - 1) + [(ydim, ydim)])
    total = total + zpad[..., 2 * ydim:] + zpad[..., :-2 * ydim]
    ypad = jnp.pad(field, [(0, 0)] * (rank - 1) + [(1, 1)])
    column = jnp.arange(zdim * ydim) % ydim
    upper = (column != ydim - 1).astype(jnp.float32)
    lower = (column != 0).astype(jnp.float32)
    return total + upper * ypad[..., 2:] + lower * ypad[..., :-2]

def edge_weights(xdim, left, right):
    position = jnp.arange(xdim)[:, None]
    return left * (position == 0).astype(jnp.float32) + right * (position == xdim - 1).astype(jnp.float32)

def smooth(field, target, diag, scale, zdim, ydim, sweeps):
    for sweep in range(sweeps):
        applied = diag * field - scale * neighbour_sum(field, zdim, ydim)
        field = field + DAMPING * (target - applied) / diag
    return field

def restrict(field, zdim, ydim):
    modes, groups, xdim, plane = field.shape
    blocks = field.reshape(modes, groups, xdim // 2, 2, zdim // 2, 2, ydim // 2, 2)
    return jnp.mean(blocks, axis=(3, 5, 7)).reshape(modes, groups, xdim // 2, zdim // 2 * (ydim // 2))

def prolong(field, zdim, ydim):
    modes, groups, xdim, plane = field.shape
    spread = field.reshape(modes, groups, xdim, 1, zdim // 2, 1, ydim // 2, 1)
    spread = jnp.broadcast_to(spread, (modes, groups, xdim, 2, zdim // 2, 2, ydim // 2, 2))
    return spread.reshape(modes, groups, 2 * xdim, zdim * ydim)

def vcycle(field, target, shifts, left, right, level, zdim, ydim):
    scale = 0.25 ** level
    edge = edge_weights(field.shape[2], left, right)
    diag = shifts + scale * (6.0 + edge)
    if level == LEVELS - 1:
        return smooth(field, target, diag, scale, zdim, ydim, 6)
    field = smooth(field, target, diag, scale, zdim, ydim, 2)
    resid = target - (diag * field - scale * neighbour_sum(field, zdim, ydim))
    coarse_target = restrict(resid, zdim, ydim)
    coarse = vcycle(jnp.zeros_like(coarse_target), coarse_target, shifts, left, right, level + 1, zdim // 2, ydim // 2)
    field = field + prolong(coarse, zdim, ydim)
    return smooth(field, target, diag, scale, zdim, ydim, 2)

def solve_modes(target, shifts, left, right):
    field = jnp.zeros_like(target)
    for cycle in range(CYCLES):
        field = vcycle(field, target, shifts, left, right, 0, CZ, CY)
    return field

def reference(source, previous, time_modes, time_back, step_code):
    steps, cells_x, plane = source.shape
    groups = N_GX
    src = source.reshape(steps, groups, CX, plane)
    prev = previous.reshape(steps, groups, CX, plane)
    index = jnp.arange(groups)
    has_left = (index > 0).astype(jnp.float32)
    has_right = (index < groups - 1).astype(jnp.float32)
    left_near = jnp.pad(prev[:, :-1, -1, :], ((0, 0), (1, 0), (0, 0)))
    right_near = jnp.pad(prev[:, 1:, 0, :], ((0, 0), (0, 1), (0, 0)))
    trace_left = has_left[None, :, None] * (left_near - ROBIN * prev[:, :, 0, :])
    trace_right = has_right[None, :, None] * (right_near - ROBIN * prev[:, :, -1, :])
    rhs = src.at[:, :, 0, :].add(trace_left).at[:, :, -1, :].add(trace_right)
    modes = jnp.einsum('mt,tgxc->mgxc', time_modes, rhs, precision=lax.Precision.HIGHEST)
    shifts = (0.05 * jnp.exp2(step_code.astype(jnp.float32) / 4.0)).reshape(steps, 1, 1, 1)
    left = (ROBIN * has_left).reshape(1, groups, 1, 1)
    right = (ROBIN * has_right).reshape(1, groups, 1, 1)
    solved = solve_modes(modes, shifts, left, right)
    result = jnp.einsum('tm,mgxc->tgxc', time_back, solved, precision=lax.Precision.HIGHEST)
    return result.reshape(steps, cells_x, plane)
```

```python
import functools

import jax
import jax.numpy as jnp
from jax import lax
from jax.experimental import pallas as pl
from jax.experimental.pallas import tpu as pltpu
from jax.sharding import PartitionSpec as P

CYCLES = 2
ROBIN = 1.0
DAMPING = 0.8
LANES = 128
PLANES = 32
TILES = 4
UNROLL = 4

CHUNKS = ((0, 16),)
DEPTH = PLANES // (2 * len(CHUNKS))


def pack_kernel(starts, edges, *refs):
    if edges:
        source_ref, low_ref, high_ref, first_ref, last_ref, out_ref = refs
    else:
        source_ref, out_ref = refs
    steps = source_ref.shape[0]
    for i, start in enumerate(starts):
        for tile in range(TILES):
            peer = i * TILES + tile
            cells = pl.ds(tile * LANES, LANES)
            for t in range(steps):
                for row in range(0, DEPTH, 8):
                    out_ref[pl.ds((peer * DEPTH + row) * steps + t, 8, stride=steps), :] = source_ref[
                        t, pl.ds(start + row, 8), cells
                    ]
    if edges:
        group = lax.axis_index("gx")
        left = (group > 0).astype(jnp.float32)
        right = (group < lax.axis_size("gx") - 1).astype(jnp.float32)
        for i, start in enumerate(starts):
            for tile in range(TILES):
                cells = pl.ds(tile * LANES, LANES)
                peer = i * TILES + tile
                if start == 0:
                    rows = pl.ds(peer * DEPTH * steps, steps)
                    out_ref[rows, :] += left * (low_ref[:, cells] - ROBIN * first_ref[:, cells])
                if start + DEPTH == PLANES:
                    rows = pl.ds((peer * DEPTH + DEPTH - 1) * steps, steps)
                    out_ref[rows, :] += right * (high_ref[:, cells] - ROBIN * last_ref[:, cells])


def unpack_kernel(*refs):
    *in_refs, out_ref = refs
    steps = out_ref.shape[0]
    for starts, in_ref in zip(CHUNKS, in_refs):
        for i, start in enumerate(starts):
            for tile in range(TILES):
                peer = i * TILES + tile
                for t in range(steps):
                    for row in range(0, DEPTH, 8):
                        out_ref[t, pl.ds(start + row, 8), pl.ds(tile * LANES, LANES)] = in_ref[
                            pl.ds((peer * DEPTH + row) * steps + t, 8, stride=steps), :
                        ]


def halves(value):
    high = value.astype(jnp.bfloat16)
    return high, (value - high.astype(jnp.float32)).astype(jnp.bfloat16)


def product_kernel(matrix_ref, in_ref, out_ref):
    size = matrix_ref.shape[0]
    high, low = halves(matrix_ref[...])
    left = jnp.concatenate(
        [jnp.concatenate([high, high], axis=1), jnp.concatenate([low, low], axis=1)], axis=0
    )
    block = in_ref.shape[2]
    for x in range(0, DEPTH, 2):
        right = jnp.concatenate(
            [in_ref[:, x + k].reshape(size, LANES) for k in range(2)], axis=1
        )
        high, low = halves(right)
        total = jnp.dot(
            left, jnp.concatenate([high, low], axis=0), preferred_element_type=jnp.float32
        )
        total = total[:size] + total[size:]
        for k in range(2):
            out_ref[:, x + k] = total[:, k * LANES : (k + 1) * LANES].reshape(
                size // block, block, LANES
            )


def solver_kernel(*refs):
    n = len(CHUNKS)
    code_ref, *rest = refs
    f_refs, out_refs = rest[:n], rest[n : 2 * n]
    v_ref, w_ref, d_ref, f1_ref, v1_ref, w1_ref, d1_ref = rest[2 * n :]
    modes = v_ref.shape[2]
    shape = (modes, LANES)
    lane = lax.broadcasted_iota(jnp.int32, shape, 1)
    mode = lax.broadcasted_iota(jnp.int32, shape, 0)
    zero = jnp.zeros(shape, jnp.float32)
    code = jnp.zeros(shape, jnp.int32)
    for m in range(modes):
        code = jnp.where(mode == m, code_ref[m], code)
    shift = 0.05 * jnp.exp2(code.astype(jnp.float32) / 4.0)
    group = lax.axis_index("gx")
    left = ROBIN * (group > 0).astype(jnp.float32)
    right = ROBIN * (group < lax.axis_size("gx") - 1).astype(jnp.float32)

    def edge_of(x, count):
        return (left if x == 0 else 0.0) + (right if x == count - 1 else 0.0)

    for x in range(PLANES):
        if x in (0, PLANES - 1) or x == 1:
            diag = shift + (6.0 + edge_of(x, PLANES))
            weight = DAMPING / diag
        d_ref[x] = diag
        w_ref[x] = weight
    for x in range(PLANES // 2):
        if x in (0, PLANES // 2 - 1) or x == 1:
            diag = shift + 0.25 * (6.0 + edge_of(x, PLANES // 2))
            weight = DAMPING / diag
        d1_ref[x] = diag
        w1_ref[x] = weight

    segments = []
    for f_ref, out_ref, starts in zip(f_refs, out_refs, CHUNKS):
        for i, start in enumerate(starts):
            segments.append((start, i, f_ref, out_ref))
    segments.sort(key=lambda s: s[0])

    roll = lambda value, by: pltpu.roll(value, by % LANES, 1)
    low_half = lane < 64
    y_first = lane % 64 == 0
    y_last = lane % 64 == 63

    def neighbours(before, here, after):
        turned = [roll(v, 64) for v in here]
        sums = []
        for c in range(TILES):
            total = before[c] + after[c] + turned[c]
            down = turned[c - 1] if c > 0 else zero
            up = turned[c + 1] if c < TILES - 1 else zero
            total = total + jnp.where(low_half, down, up)
            total = total + jnp.where(y_first, zero, roll(here[c], 1))
            total = total + jnp.where(y_last, zero, roll(here[c], -1))
            sums.append(total)
        return sums

    def march(plane_at, work, unroll):
        carry = [zero] * TILES, plane_at(0, 0, 0)
        for s in range(len(segments)):
            last = s == len(segments) - 1

            def body(step, carry, s=s, last=last, final=False):
                before, here = carry
                window = [before, here]
                for u in range(unroll):
                    x = step * unroll + u + 1
                    if final and u == unroll - 1:
                        window.append([zero] * TILES if last else plane_at(s + 1, 0, 0))
                    else:
                        window.append(plane_at(s, x, u + 1))
                work(s, step * unroll, window)
                return window[-2], window[-1]

            carry = lax.fori_loop(0, DEPTH // unroll - 1, body, carry)
            carry = body(DEPTH // unroll - 1, carry, final=True)

    def right_side(s, x):
        _, i, f_ref, _ = segments[s]
        return [f_ref[i * TILES + c, x] for c in range(TILES)]

    def field(s, x, u):
        start = segments[s][0]
        return [v_ref[start + x, c * modes // modes] if False else v_ref[start + x, c] for c in range(TILES)]

    def scaled(s, x, u):
        start = segments[s][0]
        weight = w_ref[start + x]
        return [weight * f for f in right_side(s, x)]

    def corrected(s, x, u):
        start = segments[s][0]
        coarse = v1_ref[(start + x) // 2]
        return [
            v_ref[start + x, c]
            + jnp.take_along_axis(coarse, c * 32 + lane % 64 // 2, axis=1)
            for c in range(TILES)
        ]

    def sweep(final):
        def work(s, x, window):
            start, i, _, out_ref = segments[s]
            for u in range(len(window) - 2):
                before, here, after = window[u : u + 3]
                weight = w_ref[start + x + u]
                sums = neighbours(before, here, after)
                f = right_side(s, x + u)
                for c in range(TILES):
                    value = (1.0 - DAMPING) * here[c] + weight * (f[c] + sums[c])
                    if final:
                        out_ref[i * TILES + c, x + u] = value
                    else:
                        v_ref[start + x + u, c] = value

        return work

    def residual(s, x, window):
        start = segments[s][0]
        planes = []
        for u in range(len(window) - 2):
            before, here, after = window[u : u + 3]
            diag = d_ref[start + x + u]
            sums = neighbours(before, here, after)
            f = right_side(s, x + u)
            planes.append([f[c] - (diag * here[c] - sums[c]) for c in range(TILES)])
        for u in range(0, len(planes), 2):
            pair = [planes[u][c] + planes[u + 1][c] for c in range(TILES)]
            parts = []
            for c in (0, 2):
                both = jnp.where(low_half, pair[c], pair[c + 1]) + roll(
                    jnp.where(low_half, pair[c + 1], pair[c]), 64
                )
                both = both + roll(both, -1)
                parts.append(
                    jnp.take_along_axis(both, lane % 64 // 32 * 64 + lane % 32 * 2, axis=1)
                )
            f1_ref[(start + x + u) // 2] = 0.125 * jnp.where(low_half, parts[0], parts[1])

    z_first = lane < 32
    z_last = lane >= 96
    y1_first = lane % 32 == 0
    y1_last = lane % 32 == 31
    half = PLANES // 2

    def neighbours1(before, here, after):
        total = before + after
        total = total + jnp.where(z_first, zero, roll(here, 32))
        total = total + jnp.where(z_last, zero, roll(here, -32))
        total = total + jnp.where(y1_first, zero, roll(here, 1))
        return total + jnp.where(y1_last, zero, roll(here, -1))

    def march1(plane_at, work):
        before, here = zero, plane_at(0)
        for x in range(half):
            after = plane_at(x + 1) if x + 1 < half else zero
            work(x, before, here, after)
            before, here = here, after

    def sweep1(x, before, here, after):
        total = f1_ref[x] + 0.25 * neighbours1(before, here, after)
        v1_ref[x] = (1.0 - DAMPING) * here + w1_ref[x] * total

    used = lane < 32
    quarter = half // 2
    y2_first = lane % 16 == 0
    y2_last = lane % 16 == 15

    def coarsest(f2):
        weights = []
        for x in range(quarter):
            if x in (0, quarter - 1) or x == 1:
                diag = shift + 0.0625 * (6.0 + edge_of(x, quarter))
                weight = jnp.where(used, DAMPING / diag, zero)
            weights.append(weight)
        g = [weights[x] * f2[x] for x in range(quarter)]
        v = g
        for _ in range(5):
            new = []
            for x in range(quarter):
                total = (v[x - 1] if x > 0 else zero) + (v[x + 1] if x < quarter - 1 else zero)
                total = total + roll(v[x], 16) + roll(v[x], -16)
                total = total + jnp.where(y2_first, zero, roll(v[x], 1))
                total = total + jnp.where(y2_last, zero, roll(v[x], -1))
                new.append((1.0 - DAMPING) * v[x] + g[x] + (0.0625 * weights[x]) * total)
            v = new
        return v

    def level1():
        march1(lambda x: w1_ref[x] * f1_ref[x], sweep1)
        r1 = [None] * half

        def residual1(x, before, here, after):
            r1[x] = f1_ref[x] - (d1_ref[x] * here - 0.25 * neighbours1(before, here, after))

        march1(lambda x: v1_ref[x], residual1)
        f2 = []
        for x in range(quarter):
            pair = r1[2 * x] + r1[2 * x + 1]
            pair = pair + roll(pair, -32)
            pair = pair + roll(pair, -1)
            picked = jnp.take_along_axis(pair, lane % 32 // 16 * 64 + lane % 16 * 2, axis=1)
            f2.append(jnp.where(used, 0.125 * picked, zero))
        v2 = coarsest(f2)
        spread = [
            jnp.take_along_axis(v, lane // 64 * 16 + lane % 32 // 2, axis=1) for v in v2
        ]
        march1(lambda x: v1_ref[x] + spread[x // 2], sweep1)
        march1(lambda x: v1_ref[x], sweep1)

    for cycle in range(CYCLES):
        if cycle == 0:
            march(scaled, sweep(False), UNROLL)
        else:
            march(field, sweep(False), UNROLL)
            march(field, sweep(False), UNROLL)
        march(field, residual, UNROLL)
        level1()
        march(corrected, sweep(False), UNROLL)
        march(field, sweep(cycle == CYCLES - 1), UNROLL)


def vmem(count):
    return [pl.BlockSpec(memory_space=pltpu.VMEM)] * count


def body(source, previous, time_modes, time_back, step_code):
    steps = source.shape[0]
    peers = lax.axis_size("ta")
    count = lax.axis_size("gx")
    first, last = previous[:, 0, :], previous[:, PLANES - 1, :]
    forward = [(i, i + 1) for i in range(count - 1)]
    low = lax.ppermute(last, "gx", forward)
    high = lax.ppermute(first, "gx", [(b, a) for a, b in forward])
    shape = jax.ShapeDtypeStruct((peers, DEPTH, steps, LANES), jnp.float32)
    flat = jax.ShapeDtypeStruct((peers * DEPTH * steps, LANES), jnp.float32)

    def exchange(value):
        return lax.all_to_all(value, "ta", split_axis=0, concat_axis=0, tiled=True)

    def product(matrix, value):
        return pl.pallas_call(
            product_kernel, out_shape=shape, in_specs=vmem(2), out_specs=vmem(1)[0]
        )(matrix, value)

    modes = []
    for starts in CHUNKS:
        edges = 0 in starts
        extra = (low, high, first, last) if edges else ()
        packed = pl.pallas_call(
            functools.partial(pack_kernel, starts, edges),
            out_shape=flat,
            in_specs=vmem(1 + len(extra)),
            out_specs=vmem(1)[0],
        )(source, *extra)
        modes.append(exchange(product(time_modes, exchange(packed.reshape(shape.shape)))))
    n = len(CHUNKS)
    solved = pl.pallas_call(
        solver_kernel,
        out_shape=[shape] * n,
        in_specs=[pl.BlockSpec(memory_space=pltpu.SMEM)] + vmem(n),
        out_specs=vmem(n),
        scratch_shapes=[
            pltpu.VMEM((PLANES, TILES, steps, LANES), jnp.float32),
            pltpu.VMEM((PLANES, steps, LANES), jnp.float32),
            pltpu.VMEM((PLANES, steps, LANES), jnp.float32),
            pltpu.VMEM((PLANES // 2, steps, LANES), jnp.float32),
            pltpu.VMEM((PLANES // 2, steps, LANES), jnp.float32),
            pltpu.VMEM((PLANES // 2, steps, LANES), jnp.float32),
            pltpu.VMEM((PLANES // 2, steps, LANES), jnp.float32),
        ],
    )(step_code, *modes)
    back = [exchange(product(time_back, exchange(value))).reshape(flat.shape) for value in solved]
    return pl.pallas_call(
        unpack_kernel,
        out_shape=jax.ShapeDtypeStruct(source.shape, jnp.float32),
        in_specs=vmem(n),
        out_specs=vmem(1)[0],
    )(*back)


def solution(mesh):
    placed = (P("ta", "gx", None), P("ta", "gx", None), P(), P(), P("ta"))
    return jax.shard_map(
        body, mesh=mesh, in_specs=placed, out_specs=P("ta", "gx", None), check_vma=False
    )
```

```python
import functools

import jax
import jax.numpy as jnp
from jax import lax
from jax.experimental import pallas as pl
from jax.experimental.pallas import tpu as pltpu
from jax.sharding import PartitionSpec as P

CYCLES = 2
ROBIN = 1.0
DAMPING = 0.8
LANES = 128
SIDE = 8
HIGH = 8
LOW = 4
CZ = 8
CY = 64
TILES = 4
GROUP = 2
LIMIT = 24 * 2**20


def params():
    return pltpu.CompilerParams(vmem_limit_bytes=LIMIT)


def pack_kernel(source_ref, low_ref, high_ref, first_ref, last_ref, out_ref, turned_ref):
    steps = source_ref.shape[0]
    planes = HIGH * LOW
    for tile in range(TILES):
        cells = pl.ds(tile * LANES, LANES)
        for t in range(steps):
            for row in range(0, planes, 8):
                turned_ref[pl.ds((tile * planes + row) * steps + t, 8, stride=steps), :] = source_ref[
                    t, pl.ds(row, 8), cells
                ]
    group = lax.axis_index("gx")
    left = (group > 0).astype(jnp.float32)
    right = (group < lax.axis_size("gx") - 1).astype(jnp.float32)
    for half in range(2):
        for tile in range(TILES):
            cells = pl.ds(tile * LANES, LANES)
            for low in range(2):
                for high in range(HIGH):
                    x = high * LOW + 2 * half + low
                    value = turned_ref[pl.ds((tile * planes + x) * steps, steps), :]
                    if x == 0:
                        value += left * (low_ref[:, cells] - ROBIN * first_ref[:, cells])
                    if x == planes - 1:
                        value += right * (high_ref[:, cells] - ROBIN * last_ref[:, cells])
                    out_ref[half * TILES + tile, low * HIGH + high] = value


def unpack_kernel(in_ref, out_ref, turned_ref):
    steps = out_ref.shape[0]
    planes = HIGH * LOW
    for half in range(2):
        for tile in range(TILES):
            for low in range(2):
                for high in range(HIGH):
                    x = high * LOW + 2 * half + low
                    turned_ref[pl.ds((tile * planes + x) * steps, steps), :] = in_ref[
                        half * TILES + tile, low * HIGH + high
                    ]
    for tile in range(TILES):
        for t in range(steps):
            for row in range(0, planes, 8):
                out_ref[t, pl.ds(row, 8), pl.ds(tile * LANES, LANES)] = turned_ref[
                    pl.ds((tile * planes + row) * steps + t, 8, stride=steps), :
                ]


def halves(value):
    high = value.astype(jnp.bfloat16)
    return high, (value - high.astype(jnp.float32)).astype(jnp.bfloat16)


def regroup(values):
    block = lax.broadcasted_iota(jnp.int32, values[0].shape, 1) // (LANES // SIDE)
    values = [values[-q % SIDE] for q in range(SIDE)]
    for bit in (1, 2, 4):
        odd = (block & bit) != 0
        values = [jnp.where(odd, values[(q - bit) % SIDE], values[q]) for q in range(SIDE)]
    return values


def forward_kernel(matrix_ref, in_ref, out_ref, mixed_ref):
    size = matrix_ref.shape[0]
    matrix = matrix_ref[...].T
    for high in range(HIGH):
        turned = pltpu.roll(matrix, high * (LANES // SIDE), 1) if high else matrix
        main, rest = halves(turned)
        right = jnp.concatenate([main, rest], axis=1)
        right = jnp.concatenate([right, right], axis=0)
        parts = [in_ref[:, low * HIGH + high].reshape(size, LANES).T for low in range(2)]
        main, rest = halves(jnp.concatenate(parts, axis=0))
        total = jnp.dot(
            jnp.concatenate([main, rest], axis=1), right, preferred_element_type=jnp.float32
        )
        mixed_ref[high] = total[:, :size] + total[:, size:]
    for row in range(0, 2 * LANES, 8):
        rows = pl.ds(row, 8)
        for owner, value in enumerate(regroup([mixed_ref[high, rows, :] for high in range(HIGH)])):
            out_ref[owner, rows, :] = value


def backward_kernel(matrix_ref, in_ref, out_ref, mixed_ref):
    size = matrix_ref.shape[0]
    block = out_ref.shape[2]
    for row in range(0, 2 * LANES, 8):
        rows = pl.ds(row, 8)
        for high, value in enumerate(regroup([in_ref[owner, rows, :] for owner in range(SIDE)])):
            mixed_ref[high, rows, :] = value
    matrix = matrix_ref[...]
    for high in range(HIGH):
        turned = pltpu.roll(matrix, high * (LANES // SIDE), 1) if high else matrix
        main, rest = halves(turned)
        left = jnp.concatenate(
            [jnp.concatenate([main, main], axis=1), jnp.concatenate([rest, rest], axis=1)], axis=0
        )
        main, rest = halves(mixed_ref[high])
        total = lax.dot_general(
            left,
            jnp.concatenate([main, rest], axis=1),
            (((1,), (1,)), ((), ())),
            preferred_element_type=jnp.float32,
        )
        total = total[:size] + total[size:]
        for low in range(2):
            out_ref[:, low * HIGH + high] = total[:, low * LANES : (low + 1) * LANES].reshape(
                size // block, block, LANES
            )


def solver_kernel(code_ref, f_ref, out_ref, *scratch):
    va, vb, spread_ref, f1_ref, v1a, v1b, spread1_ref, f2_ref, v2a, v2b = scratch
    shape = (8, LANES)
    lane = lax.broadcasted_iota(jnp.int32, shape, 1)
    modes = LANES // SIDE
    zero = jnp.zeros(shape, jnp.float32)
    code = jnp.zeros(shape, jnp.int32)
    for m in range(modes):
        code = jnp.where(lane % modes == m, code_ref[m], code)
    shift = 0.05 * jnp.exp2(code.astype(jnp.float32) / 4.0)
    group = lax.axis_index("gx")
    has_left = ROBIN * (group > 0).astype(jnp.float32)
    has_right = ROBIN * (group < lax.axis_size("gx") - 1).astype(jnp.float32)
    high = (lane // modes - lax.axis_index("ta") + SIDE) % SIDE
    x_first = high == 0
    x_last = high == SIDE - 1
    left = jnp.where(x_first, has_left, zero)
    right = jnp.where(x_last, has_right, zero)

    class Level:
        def __init__(self, level, field, other, right_side, low, cz, cy):
            self.scale = 0.25**level
            self.fields = (field, other)
            self.right_side = right_side
            self.low, self.cz, self.cy = low, cz, cy
            self.pitch = cy + 8
            self.diag, self.weight = [], []
            for x in range(low):
                edge = 6.0 + (left if x == 0 else zero)
                if x == low - 1:
                    edge = edge + right
                self.diag.append(shift + self.scale * edge)
                self.weight.append(DAMPING / self.diag[-1])
            for ref in self.fields:
                for k in range(low * cz + 1):
                    ref[pl.ds(k * self.pitch, 8), :] = zero

        def base(self, x, z):
            return 8 + (x * self.cz + z) * self.pitch

        def load(self, ref, x, z, row):
            return ref[pl.ds(self.base(x, z) + row, 8), :]

        def store(self, ref, x, z, row, value):
            ref[pl.ds(self.base(x, z) + row, 8), :] = value

        def sums(self, ref, row):
            here = [[self.load(ref, x, z, row) for z in range(self.cz)] for x in range(self.low)]
            step = LANES // SIDE
            wrap_low = [pltpu.roll(here[-1][z], step, 1) for z in range(self.cz)]
            wrap_high = [pltpu.roll(here[0][z], LANES - step, 1) for z in range(self.cz)]
            for x in range(self.low):
                for z in range(self.cz):
                    total = self.load(ref, x, z, row - 1) + self.load(ref, x, z, row + 1)
                    if z > 0:
                        total = total + here[x][z - 1]
                    if z < self.cz - 1:
                        total = total + here[x][z + 1]
                    if x > 0:
                        total = total + here[x - 1][z]
                    if x < self.low - 1:
                        total = total + here[x + 1][z]
                    if x == 0:
                        total = total + jnp.where(x_first, zero, wrap_low[z])
                    if x == self.low - 1:
                        total = total + jnp.where(x_last, zero, wrap_high[z])
                    if self.scale != 1.0:
                        total = self.scale * total
                    yield x, z, here[x][z], total

        def over_rows(self, work):
            size = min(8 * GROUP, self.cy)
            if size == self.cy:
                for row in range(0, size, 8):
                    work(row)
                return

            def body(step, carry):
                for k in range(0, size, 8):
                    work(pl.multiple_of(step * size, 8) + k)
                return carry

            lax.fori_loop(0, self.cy // size, body, 0)

        def start(self, ref):
            def work(row):
                for x in range(self.low):
                    for z in range(self.cz):
                        self.store(ref, x, z, row, self.weight[x] * self.right_side(x, z, row))

            self.over_rows(work)

        def sweep(self, source, target=None, emit=None):
            def work(row):
                for x, z, here, total in self.sums(source, row):
                    f = self.right_side(x, z, row)
                    value = (1.0 - DAMPING) * here + self.weight[x] * (f + total)
                    if emit is None:
                        self.store(target, x, z, row, value)
                    else:
                        emit(x, z, row, value)

            self.over_rows(work)

        def residual(self, ref, spread, coarse_f):
            def work(row):
                parts = {}
                for x, z, here, total in self.sums(ref, row):
                    f = self.right_side(x, z, row)
                    value = f - (self.diag[x] * here - total)
                    key = (x // 2, z // 2)
                    parts[key] = parts[key] + value if key in parts else value
                for (x, z), value in parts.items():
                    spread[pl.ds((x * (self.cz // 2) + z) * self.cy + row, 8), :] = value

            self.over_rows(work)
            for k in range(max(self.low // 2, 1) * self.cz // 2):
                for row in range(0, self.cy // 2, 8):
                    start = k * self.cy + 2 * row
                    coarse_f[pl.ds(k * (self.cy // 2) + row, 8), :] = 0.125 * (
                        spread[pl.ds(start, 8, stride=2), :]
                        + spread[pl.ds(start + 1, 8, stride=2), :]
                    )

        def correct(self, ref, spread, coarse, coarse_ref):
            for x in range(coarse.low):
                for z in range(coarse.cz):
                    for row in range(0, coarse.cy, 8):
                        value = coarse.load(coarse_ref, x, z, row)
                        start = (x * coarse.cz + z) * self.cy + 2 * row
                        spread[pl.ds(start, 8, stride=2), :] = value
                        spread[pl.ds(start + 1, 8, stride=2), :] = value

            def work(row):
                for x in range(self.low):
                    for z in range(self.cz):
                        k = (x * coarse.low // self.low) * coarse.cz + z // 2
                        value = spread[pl.ds(k * self.cy + row, 8), :]
                        self.store(ref, x, z, row, self.load(ref, x, z, row) + value)

            self.over_rows(work)

    def fine_rows(x, z, row):
        return (x // 2) * TILES + z // 2, pl.ds((x % 2) * LANES + (z % 2) * CY + row, 8)

    def fine_f(x, z, row):
        peer, rows = fine_rows(x, z, row)
        return f_ref[peer, rows, :]

    def emit(x, z, row, value):
        peer, rows = fine_rows(x, z, row)
        out_ref[peer, rows, :] = value

    def coarse_f(ref, cz, cy):
        return lambda x, z, row: ref[pl.ds((x * cz + z) * cy + row, 8), :]

    fine = Level(0, va, vb, fine_f, LOW, CZ, CY)
    middle = Level(1, v1a, v1b, coarse_f(f1_ref, CZ // 2, CY // 2), LOW // 2, CZ // 2, CY // 2)
    coarse = Level(2, v2a, v2b, coarse_f(f2_ref, CZ // 4, CY // 4), 1, CZ // 4, CY // 4)

    for cycle in range(CYCLES):
        if cycle == 0:
            fine.start(vb)
            fine.sweep(vb, va)
        else:
            fine.sweep(va, vb)
            fine.sweep(vb, va)
        fine.residual(va, spread_ref, f1_ref)
        middle.start(v1b)
        middle.sweep(v1b, v1a)
        middle.residual(v1a, spread1_ref, f2_ref)
        coarse.start(v2a)
        for _ in range(2):
            coarse.sweep(v2a, v2b)
            coarse.sweep(v2b, v2a)
        coarse.sweep(v2a, v2b)
        middle.correct(v1a, spread1_ref, coarse, v2b)
        middle.sweep(v1a, v1b)
        middle.sweep(v1b, v1a)
        fine.correct(va, spread_ref, middle, v1a)
        fine.sweep(va, vb)
        if cycle == CYCLES - 1:
            fine.sweep(vb, emit=emit)
        else:
            fine.sweep(vb, va)


def vmem(count):
    return [pl.BlockSpec(memory_space=pltpu.VMEM)] * count


def rows(count):
    return pltpu.VMEM((count, LANES), jnp.float32)


def body(source, previous, time_modes, time_back, step_code):
    steps, planes, _ = source.shape
    peers = lax.axis_size("ta")
    count = lax.axis_size("gx")
    first, last = previous[:, 0, :], previous[:, planes - 1, :]
    forward = [(i, i + 1) for i in range(count - 1)]
    low = lax.ppermute(last, "gx", forward)
    high = lax.ppermute(first, "gx", [(b, a) for a, b in forward])
    by_step = jax.ShapeDtypeStruct((peers, planes // 2, steps, LANES), jnp.float32)
    by_mode = jax.ShapeDtypeStruct((peers, 2 * LANES, LANES), jnp.float32)
    mixed = pltpu.VMEM((HIGH, 2 * LANES, LANES), jnp.float32)
    turned = rows(TILES * planes * steps)

    def exchange(value):
        return lax.all_to_all(value, "ta", split_axis=0, concat_axis=0, tiled=True)

    def call(kernel, shape, count, *scratch):
        return pl.pallas_call(
            kernel,
            out_shape=shape,
            in_specs=vmem(count),
            out_specs=vmem(1)[0],
            scratch_shapes=scratch,
            compiler_params=params(),
        )

    packed = call(pack_kernel, by_step, 5, turned)(source, low, high, first, last)
    modes = exchange(call(forward_kernel, by_mode, 2, mixed)(time_modes, exchange(packed)))
    solved = pl.pallas_call(
        solver_kernel,
        out_shape=by_mode,
        in_specs=[pl.BlockSpec(memory_space=pltpu.SMEM)] + vmem(1),
        out_specs=vmem(1)[0],
        scratch_shapes=[
            *[rows(8 + LOW * CZ * (CY + 8))] * 2,
            rows(LOW * CZ // 4 * CY),
            rows(LOW * CZ // 4 * CY // 2),
            *[rows(8 + LOW * CZ // 4 * (CY // 2 + 8))] * 2,
            rows(CZ // 4 * CY // 2),
            rows(CZ // 4 * CY // 4),
            *[rows(8 + CZ // 4 * (CY // 4 + 8))] * 2,
        ],
        compiler_params=params(),
    )(step_code, modes)
    mixed_back = call(backward_kernel, by_step, 2, mixed)(time_back, exchange(solved))
    out = jax.ShapeDtypeStruct(source.shape, jnp.float32)
    return call(unpack_kernel, out, 1, turned)(exchange(mixed_back))


def solution(mesh):
    placed = (P("ta", "gx", None), P("ta", "gx", None), P(), P(), P("ta"))
    return jax.shard_map(
        body, mesh=mesh, in_specs=placed, out_specs=P("ta", "gx", None), check_vma=False
    )
```

```python
import jax
import jax.numpy as jnp
from jax import lax
from jax.experimental import pallas as pl
from jax.experimental.pallas import tpu as pltpu
from jax.sharding import PartitionSpec as P


CYCLES = 2
ROBIN = 1.0
DAMPING = 0.8
LANES = 128
SIDE = 8
HIGH = 8
LOW = 4
CZ = 8
CY = 64
TILES = 4
GROUP = 4
LIMIT = 24 * 2**20
PAUSE = 1800


def has_neighbours():
    group = lax.axis_index("gx")
    left = (group > 0).astype(jnp.float32)
    return left, (group < lax.axis_size("gx") - 1).astype(jnp.float32)


def turn_kernel(source_ref, first_ref, last_ref, turned_ref):
    steps = source_ref.shape[0]
    planes = HIGH * LOW
    left, right = has_neighbours()
    for tile in range(TILES):
        cells = pl.ds(tile * LANES, LANES)
        for t in range(steps):
            for row in range(0, planes, 8):
                turned_ref[pl.ds((tile * planes + row) * steps + t, 8, stride=steps), :] = source_ref[
                    t, pl.ds(row, 8), cells
                ]
        turned_ref[pl.ds(tile * planes * steps, steps), :] -= (left * ROBIN) * first_ref[:, cells]
        turned_ref[pl.ds((tile * planes + planes - 1) * steps, steps), :] -= (
            right * ROBIN
        ) * last_ref[:, cells]


def pack_kernel(turned_ref, outer_ref, inner_ref, out_ref, pause_ref):
    steps = out_ref.shape[2]
    planes = HIGH * LOW
    left, right = has_neighbours()
    odd = lax.axis_index("gx") % 2 == 1
    for half in range(2):
        for tile in range(TILES):
            cells = pl.ds(tile * LANES, LANES)
            outer, inner = outer_ref[:, cells], inner_ref[:, cells]
            for low in range(2):
                for high in range(HIGH):
                    x = high * LOW + 2 * half + low
                    value = turned_ref[pl.ds((tile * planes + x) * steps, steps), :]
                    if x == 0:
                        value += left * jnp.where(odd, inner, outer)
                    if x == planes - 1:
                        value += right * jnp.where(odd, outer, inner)
                    out_ref[half * TILES + tile, low * HIGH + high] = value
    late = lax.axis_index("gx") % 2
    pause_ref[...] = lax.fori_loop(
        0, late * PAUSE, lambda _, value: pltpu.roll(value, 1, 1), out_ref[0, 0, :8, :]
    )


def unpack_kernel(in_ref, out_ref, turned_ref):
    steps = out_ref.shape[0]
    planes = HIGH * LOW
    for half in range(2):
        for tile in range(TILES):
            for low in range(2):
                for high in range(HIGH):
                    x = high * LOW + 2 * half + low
                    turned_ref[pl.ds((tile * planes + x) * steps, steps), :] = in_ref[
                        half * TILES + tile, low * HIGH + high
                    ]
    for tile in range(TILES):
        for t in range(steps):
            for row in range(0, planes, 8):
                out_ref[t, pl.ds(row, 8), pl.ds(tile * LANES, LANES)] = turned_ref[
                    pl.ds((tile * planes + row) * steps + t, 8, stride=steps), :
                ]


def halves(value):
    high = value.astype(jnp.bfloat16)
    return high, (value - high.astype(jnp.float32)).astype(jnp.bfloat16)


def regroup(values):
    block = lax.broadcasted_iota(jnp.int32, values[0].shape, 1) // (LANES // SIDE)
    values = [values[-q % SIDE] for q in range(SIDE)]
    for bit in (1, 2, 4):
        odd = (block & bit) != 0
        values = [jnp.where(odd, values[(q - bit) % SIDE], values[q]) for q in range(SIDE)]
    return values


def forward_kernel(matrix_ref, in_ref, out_ref, mixed_ref):
    size = matrix_ref.shape[0]
    matrix = matrix_ref[...].T
    for high in range(HIGH):
        turned = pltpu.roll(matrix, high * (LANES // SIDE), 1) if high else matrix
        main, rest = halves(turned)
        right = jnp.concatenate([main, rest], axis=1)
        right = jnp.concatenate([right, right], axis=0)
        parts = [in_ref[:, low * HIGH + high].reshape(size, LANES).T for low in range(2)]
        main, rest = halves(jnp.concatenate(parts, axis=0))
        total = jnp.dot(
            jnp.concatenate([main, rest], axis=1), right, preferred_element_type=jnp.float32
        )
        mixed_ref[high] = total[:, :size] + total[:, size:]
    for row in range(0, 2 * LANES, 8):
        rows = pl.ds(row, 8)
        for owner, value in enumerate(regroup([mixed_ref[high, rows, :] for high in range(HIGH)])):
            out_ref[owner, rows, :] = value


def backward_kernel(matrix_ref, in_ref, out_ref, mixed_ref):
    size = matrix_ref.shape[0]
    block = out_ref.shape[2]
    for row in range(0, 2 * LANES, 8):
        rows = pl.ds(row, 8)
        for high, value in enumerate(regroup([in_ref[owner, rows, :] for owner in range(SIDE)])):
            mixed_ref[high, rows, :] = value
    matrix = matrix_ref[...]
    for high in range(HIGH):
        turned = pltpu.roll(matrix, high * (LANES // SIDE), 1) if high else matrix
        main, rest = halves(turned)
        left = jnp.concatenate(
            [jnp.concatenate([main, main], axis=1), jnp.concatenate([rest, rest], axis=1)], axis=0
        )
        main, rest = halves(mixed_ref[high])
        total = lax.dot_general(
            left,
            jnp.concatenate([main, rest], axis=1),
            (((1,), (1,)), ((), ())),
            preferred_element_type=jnp.float32,
        )
        total = total[:size] + total[size:]
        for low in range(2):
            out_ref[:, low * HIGH + high] = total[:, low * LANES : (low + 1) * LANES].reshape(
                size // block, block, LANES
            )


def solver_kernel(code_ref, f_ref, out_ref, *scratch):
    va, vb, spread_ref, f1_ref, v1a, v1b, spread1_ref, f2_ref, v2a, v2b = scratch
    shape = (8, LANES)
    lane = lax.broadcasted_iota(jnp.int32, shape, 1)
    modes = LANES // SIDE
    zero = jnp.zeros(shape, jnp.float32)
    code = jnp.zeros(shape, jnp.int32)
    for m in range(modes):
        code = jnp.where(lane % modes == m, code_ref[m], code)
    shift = 0.05 * jnp.exp2(code.astype(jnp.float32) / 4.0)
    has_left, has_right = (ROBIN * side for side in has_neighbours())
    high = (lane // modes - lax.axis_index("ta") + SIDE) % SIDE
    x_first = high == 0
    x_last = high == SIDE - 1
    left = jnp.where(x_first, has_left, zero)
    right = jnp.where(x_last, has_right, zero)

    class Level:
        def __init__(self, level, field, other, right_side, low, cz, cy):
            self.scale = 0.25**level
            self.fields = (field, other)
            self.right_side = right_side
            self.low, self.cz, self.cy = low, cz, cy
            self.pitch = cy + 8
            self.diag, self.weight = [], []
            for x in range(low):
                edge = 6.0 + (left if x == 0 else zero)
                if x == low - 1:
                    edge = edge + right
                self.diag.append(shift + self.scale * edge)
                self.weight.append(DAMPING / self.diag[-1])
            for ref in self.fields:
                for k in range(low * cz + 1):
                    ref[pl.ds(k * self.pitch, 8), :] = zero

        def base(self, x, z):
            return 8 + (x * self.cz + z) * self.pitch

        def load(self, ref, x, z, row):
            return ref[pl.ds(self.base(x, z) + row, 8), :]

        def store(self, ref, x, z, row, value):
            ref[pl.ds(self.base(x, z) + row, 8), :] = value

        def sums(self, ref, row):
            here = [[self.load(ref, x, z, row) for z in range(self.cz)] for x in range(self.low)]
            step = LANES // SIDE
            wrap_low = [pltpu.roll(here[-1][z], step, 1) for z in range(self.cz)]
            wrap_high = [pltpu.roll(here[0][z], LANES - step, 1) for z in range(self.cz)]
            for x in range(self.low):
                for z in range(self.cz):
                    total = self.load(ref, x, z, row - 1) + self.load(ref, x, z, row + 1)
                    if z > 0:
                        total = total + here[x][z - 1]
                    if z < self.cz - 1:
                        total = total + here[x][z + 1]
                    if x > 0:
                        total = total + here[x - 1][z]
                    if x < self.low - 1:
                        total = total + here[x + 1][z]
                    if x == 0:
                        total = total + jnp.where(x_first, zero, wrap_low[z])
                    if x == self.low - 1:
                        total = total + jnp.where(x_last, zero, wrap_high[z])
                    if self.scale != 1.0:
                        total = self.scale * total
                    yield x, z, here[x][z], total

        def over_rows(self, work):
            size = min(8 * GROUP, self.cy) if self.scale == 1.0 else self.cy
            if size == self.cy:
                for row in range(0, size, 8):
                    work(row)
                return

            def body(step, carry):
                for k in range(0, size, 8):
                    work(pl.multiple_of(step * size, 8) + k)
                return carry

            lax.fori_loop(0, self.cy // size, body, 0)

        def start(self, ref):
            def work(row):
                for x in range(self.low):
                    for z in range(self.cz):
                        self.store(ref, x, z, row, self.weight[x] * self.right_side(x, z, row))

            self.over_rows(work)

        def sweep(self, source, target=None, emit=None):
            def work(row):
                for x, z, here, total in self.sums(source, row):
                    f = self.right_side(x, z, row)
                    value = (1.0 - DAMPING) * here + self.weight[x] * (f + total)
                    if emit is None:
                        self.store(target, x, z, row, value)
                    else:
                        emit(x, z, row, value)

            self.over_rows(work)

        def residual(self, ref, spread, coarse_f):
            def work(row):
                parts = {}
                for x, z, here, total in self.sums(ref, row):
                    f = self.right_side(x, z, row)
                    value = f - (self.diag[x] * here - total)
                    key = (x // 2, z // 2)
                    parts[key] = parts[key] + value if key in parts else value
                for (x, z), value in parts.items():
                    spread[pl.ds((x * (self.cz // 2) + z) * self.cy + row, 8), :] = value

            self.over_rows(work)
            for k in range(max(self.low // 2, 1) * self.cz // 2):
                for row in range(0, self.cy // 2, 8):
                    start = k * self.cy + 2 * row
                    coarse_f[pl.ds(k * (self.cy // 2) + row, 8), :] = 0.125 * (
                        spread[pl.ds(start, 8, stride=2), :]
                        + spread[pl.ds(start + 1, 8, stride=2), :]
                    )

        def correct(self, ref, spread, coarse, coarse_ref):
            for x in range(coarse.low):
                for z in range(coarse.cz):
                    for row in range(0, coarse.cy, 8):
                        value = coarse.load(coarse_ref, x, z, row)
                        start = (x * coarse.cz + z) * self.cy + 2 * row
                        spread[pl.ds(start, 8, stride=2), :] = value
                        spread[pl.ds(start + 1, 8, stride=2), :] = value

            def work(row):
                for x in range(self.low):
                    for z in range(self.cz):
                        k = (x * coarse.low // self.low) * coarse.cz + z // 2
                        value = spread[pl.ds(k * self.cy + row, 8), :]
                        self.store(ref, x, z, row, self.load(ref, x, z, row) + value)

            self.over_rows(work)

    def fine_rows(x, z, row):
        return (x // 2) * TILES + z // 2, pl.ds((x % 2) * LANES + (z % 2) * CY + row, 8)

    def fine_f(x, z, row):
        peer, rows = fine_rows(x, z, row)
        return f_ref[peer, rows, :]

    def emit(x, z, row, value):
        peer, rows = fine_rows(x, z, row)
        out_ref[peer, rows, :] = value

    def coarse_f(ref, cz, cy):
        return lambda x, z, row: ref[pl.ds((x * cz + z) * cy + row, 8), :]

    fine = Level(0, va, vb, fine_f, LOW, CZ, CY)
    middle = Level(1, v1a, v1b, coarse_f(f1_ref, CZ // 2, CY // 2), LOW // 2, CZ // 2, CY // 2)
    coarse = Level(2, v2a, v2b, coarse_f(f2_ref, CZ // 4, CY // 4), 1, CZ // 4, CY // 4)

    for cycle in range(CYCLES):
        if cycle == 0:
            fine.start(vb)
            fine.sweep(vb, va)
        else:
            fine.sweep(va, vb)
            fine.sweep(vb, va)
        fine.residual(va, spread_ref, f1_ref)
        middle.start(v1b)
        middle.sweep(v1b, v1a)
        middle.residual(v1a, spread1_ref, f2_ref)
        coarse.start(v2a)
        for _ in range(2):
            coarse.sweep(v2a, v2b)
            coarse.sweep(v2b, v2a)
        coarse.sweep(v2a, v2b)
        middle.correct(v1a, spread1_ref, coarse, v2b)
        middle.sweep(v1a, v1b)
        middle.sweep(v1b, v1a)
        fine.correct(va, spread_ref, middle, v1a)
        fine.sweep(va, vb)
        if cycle == CYCLES - 1:
            fine.sweep(vb, emit=emit)
        else:
            fine.sweep(vb, va)


def vmem(count):
    return [pl.BlockSpec(memory_space=pltpu.VMEM)] * count


def rows(count):
    return pltpu.VMEM((count, LANES), jnp.float32)


def exchange(value):
    return lax.all_to_all(value, "ta", split_axis=0, concat_axis=0, tiled=True)


def swaps(start, count):
    pairs = [(i, i + 1) for i in range(start, count - 1, 2)]
    return pairs + [(b, a) for a, b in pairs]


def call(kernel, shape, count, *scratch, smem=0, flops=10**6):
    return pl.pallas_call(
        kernel,
        out_shape=shape,
        in_specs=[pl.BlockSpec(memory_space=pltpu.SMEM)] * smem + vmem(count),
        out_specs=vmem(1)[0],
        scratch_shapes=scratch,
        compiler_params=pltpu.CompilerParams(vmem_limit_bytes=LIMIT),
        cost_estimate=pl.CostEstimate(flops=flops, bytes_accessed=2**20, transcendentals=0),
    )


def iteration(source, previous, time_modes, time_back, step_code):
    steps, planes, _ = source.shape
    count = lax.axis_size("gx")
    first, last = previous[:, 0, :], previous[:, planes - 1, :]
    odd = lax.axis_index("gx") % 2 == 1
    outer = lax.ppermute(jnp.where(odd, last, first), "gx", swaps(1, count))
    outer, inner = lax.optimization_barrier((outer, jnp.where(odd, first, last)))
    inner = lax.ppermute(inner, "gx", swaps(0, count))
    by_step = jax.ShapeDtypeStruct((SIDE, planes // 2, steps, LANES), jnp.float32)
    by_mode = jax.ShapeDtypeStruct((SIDE, 2 * LANES, LANES), jnp.float32)
    turned = (TILES * planes * steps, LANES)
    blocks = pltpu.VMEM((SIDE, 2 * LANES, LANES), jnp.float32)

    held = call(turn_kernel, jax.ShapeDtypeStruct(turned, jnp.float32), 3, flops=10**8)(
        source, first, last
    )
    packed = call(pack_kernel, by_step, 3, rows(8))(held, outer, inner)
    mixed = call(forward_kernel, by_mode, 2, blocks)(time_modes, exchange(packed))
    solved = call(
        solver_kernel,
        by_mode,
        1,
        *[rows(8 + LOW * CZ * (CY + 8))] * 2,
        rows(LOW * CZ // 4 * CY),
        rows(LOW * CZ // 4 * CY // 2),
        *[rows(8 + LOW * CZ // 4 * (CY // 2 + 8))] * 2,
        rows(CZ // 4 * CY // 2),
        rows(CZ // 4 * CY // 4),
        *[rows(8 + CZ // 4 * (CY // 4 + 8))] * 2,
        smem=1,
    )(step_code, exchange(mixed))
    mixed = call(backward_kernel, by_step, 2, blocks)(time_back, exchange(solved))
    result = jax.ShapeDtypeStruct(source.shape, jnp.float32)
    return call(unpack_kernel, result, 1, rows(turned[0]))(exchange(mixed))


def solution(mesh):
    placed = (P("ta", "gx", None), P("ta", "gx", None), P(), P(), P("ta"))
    return jax.shard_map(
        iteration, mesh=mesh, in_specs=placed, out_specs=P("ta", "gx", None), check_vma=False
    )
```

```python
import jax
import jax.numpy as jnp
from jax import lax
from jax.experimental import pallas as pl
from jax.experimental.pallas import tpu as pltpu
from jax.sharding import PartitionSpec as P


CYCLES = 2
ROBIN = 1.0
DAMPING = 0.8
LANES = 128
SIDE = 8
HIGH = 8
LOW = 4
CZ = 8
CY = 64
TILES = 4
GROUP = 4
LIMIT = 24 * 2**20
PAUSE = 1870


def has_neighbours():
    group = lax.axis_index("gx")
    left = (group > 0).astype(jnp.float32)
    return left, (group < lax.axis_size("gx") - 1).astype(jnp.float32)


def turn_kernel(source_ref, first_ref, last_ref, turned_ref):
    steps = source_ref.shape[0]
    planes = HIGH * LOW
    left, right = has_neighbours()
    for tile in range(TILES):
        cells = pl.ds(tile * LANES, LANES)
        for t in range(steps):
            for row in range(0, planes, 8):
                turned_ref[pl.ds((tile * planes + row) * steps + t, 8, stride=steps), :] = source_ref[
                    t, pl.ds(row, 8), cells
                ]
        turned_ref[pl.ds(tile * planes * steps, steps), :] -= (left * ROBIN) * first_ref[:, cells]
        turned_ref[pl.ds((tile * planes + planes - 1) * steps, steps), :] -= (
            right * ROBIN
        ) * last_ref[:, cells]


def pack_kernel(turned_ref, outer_ref, inner_ref, out_ref, pause_ref):
    steps = out_ref.shape[2]
    planes = HIGH * LOW
    left, right = has_neighbours()
    odd = lax.axis_index("gx") % 2 == 1
    for half in range(2):
        for tile in range(TILES):
            cells = pl.ds(tile * LANES, LANES)
            outer, inner = outer_ref[:, cells], inner_ref[:, cells]
            for low in range(2):
                for high in range(HIGH):
                    x = high * LOW + 2 * half + low
                    value = turned_ref[pl.ds((tile * planes + x) * steps, steps), :]
                    if x == 0:
                        value += left * jnp.where(odd, inner, outer)
                    if x == planes - 1:
                        value += right * jnp.where(odd, outer, inner)
                    out_ref[half * TILES + tile, low * HIGH + high] = value
    late = lax.axis_index("gx") % 2
    pause_ref[...] = lax.fori_loop(
        0, late * PAUSE, lambda _, value: pltpu.roll(value, 1, 1), out_ref[0, 0, :8, :]
    )


def unpack_kernel(in_ref, out_ref, turned_ref, stage_ref, sems):
    steps = out_ref.shape[0]
    planes = HIGH * LOW
    copies = []
    for tile in range(TILES):
        for half in range(2):
            for low in range(2):
                for high in range(HIGH):
                    x = high * LOW + 2 * half + low
                    turned_ref[pl.ds((tile * planes + x) * steps, steps), :] = in_ref[
                        half * TILES + tile, low * HIGH + high
                    ]
        for t in range(steps):
            for row in range(0, planes, 8):
                stage_ref[tile, t, pl.ds(row, 8), :] = turned_ref[
                    pl.ds((tile * planes + row) * steps + t, 8, stride=steps), :
                ]
        copies.append(
            pltpu.make_async_copy(
                stage_ref.at[tile], out_ref.at[:, :, pl.ds(tile * LANES, LANES)], sems.at[tile]
            )
        )
        copies[-1].start()
    for copy in copies:
        copy.wait()


def halves(value):
    high = value.astype(jnp.bfloat16)
    return high, (value - high.astype(jnp.float32)).astype(jnp.bfloat16)


def regroup(values):
    block = lax.broadcasted_iota(jnp.int32, values[0].shape, 1) // (LANES // SIDE)
    values = [values[-q % SIDE] for q in range(SIDE)]
    for bit in (1, 2, 4):
        odd = (block & bit) != 0
        values = [jnp.where(odd, values[(q - bit) % SIDE], values[q]) for q in range(SIDE)]
    return values


def forward_kernel(matrix_ref, in_ref, out_ref, mixed_ref):
    size = matrix_ref.shape[0]
    matrix = matrix_ref[...].T
    for high in range(HIGH):
        turned = pltpu.roll(matrix, high * (LANES // SIDE), 1) if high else matrix
        main, rest = halves(turned)
        right = jnp.concatenate([main, rest], axis=1)
        right = jnp.concatenate([right, right], axis=0)
        parts = [in_ref[:, low * HIGH + high].reshape(size, LANES).T for low in range(2)]
        main, rest = halves(jnp.concatenate(parts, axis=0))
        total = jnp.dot(
            jnp.concatenate([main, rest], axis=1), right, preferred_element_type=jnp.float32
        )
        mixed_ref[high] = total[:, :size] + total[:, size:]
    for row in range(0, 2 * LANES, 8):
        rows = pl.ds(row, 8)
        for owner, value in enumerate(regroup([mixed_ref[high, rows, :] for high in range(HIGH)])):
            out_ref[owner, rows, :] = value


def backward_kernel(matrix_ref, in_ref, out_ref, mixed_ref):
    size = matrix_ref.shape[0]
    block = out_ref.shape[2]
    for row in range(0, 2 * LANES, 8):
        rows = pl.ds(row, 8)
        for high, value in enumerate(regroup([in_ref[owner, rows, :] for owner in range(SIDE)])):
            mixed_ref[high, rows, :] = value
    matrix = matrix_ref[...]
    for high in range(HIGH):
        turned = pltpu.roll(matrix, high * (LANES // SIDE), 1) if high else matrix
        main, rest = halves(turned)
        left = jnp.concatenate(
            [jnp.concatenate([main, main], axis=1), jnp.concatenate([rest, rest], axis=1)], axis=0
        )
        main, rest = halves(mixed_ref[high])
        total = lax.dot_general(
            left,
            jnp.concatenate([main, rest], axis=1),
            (((1,), (1,)), ((), ())),
            preferred_element_type=jnp.float32,
        )
        total = total[:size] + total[size:]
        for low in range(2):
            out_ref[:, low * HIGH + high] = total[:, low * LANES : (low + 1) * LANES].reshape(
                size // block, block, LANES
            )


def solver_kernel(code_ref, f_ref, out_ref, *scratch):
    va, vb, spread_ref, f1_ref, v1a, v1b, spread1_ref, f2_ref, v2a, v2b = scratch
    shape = (8, LANES)
    lane = lax.broadcasted_iota(jnp.int32, shape, 1)
    modes = LANES // SIDE
    zero = jnp.zeros(shape, jnp.float32)
    code = jnp.zeros(shape, jnp.int32)
    for m in range(modes):
        code = jnp.where(lane % modes == m, code_ref[m], code)
    shift = 0.05 * jnp.exp2(code.astype(jnp.float32) / 4.0)
    has_left, has_right = (ROBIN * side for side in has_neighbours())
    high = (lane // modes - lax.axis_index("ta") + SIDE) % SIDE
    x_first = high == 0
    x_last = high == SIDE - 1
    left = jnp.where(x_first, has_left, zero)
    right = jnp.where(x_last, has_right, zero)

    class Level:
        def __init__(self, level, field, other, right_side, low, cz, cy):
            self.scale = 0.25**level
            self.fields = (field, other)
            self.right_side = right_side
            self.low, self.cz, self.cy = low, cz, cy
            self.pitch = cy + 8
            self.diag, self.weight = [], []
            for x in range(low):
                edge = 6.0 + (left if x == 0 else zero)
                if x == low - 1:
                    edge = edge + right
                self.diag.append(shift + self.scale * edge)
                self.weight.append(DAMPING / self.diag[-1])
            for ref in self.fields:
                for k in range(low * cz + 1):
                    ref[pl.ds(k * self.pitch, 8), :] = zero

        def base(self, x, z):
            return 8 + (x * self.cz + z) * self.pitch

        def load(self, ref, x, z, row):
            return ref[pl.ds(self.base(x, z) + row, 8), :]

        def store(self, ref, x, z, row, value):
            ref[pl.ds(self.base(x, z) + row, 8), :] = value

        def sums(self, ref, row):
            here = [[self.load(ref, x, z, row) for z in range(self.cz)] for x in range(self.low)]
            step = LANES // SIDE
            wrap_low = [pltpu.roll(here[-1][z], step, 1) for z in range(self.cz)]
            wrap_high = [pltpu.roll(here[0][z], LANES - step, 1) for z in range(self.cz)]
            for x in range(self.low):
                for z in range(self.cz):
                    total = self.load(ref, x, z, row - 1) + self.load(ref, x, z, row + 1)
                    if z > 0:
                        total = total + here[x][z - 1]
                    if z < self.cz - 1:
                        total = total + here[x][z + 1]
                    if x > 0:
                        total = total + here[x - 1][z]
                    if x < self.low - 1:
                        total = total + here[x + 1][z]
                    if x == 0:
                        total = total + jnp.where(x_first, zero, wrap_low[z])
                    if x == self.low - 1:
                        total = total + jnp.where(x_last, zero, wrap_high[z])
                    if self.scale != 1.0:
                        total = self.scale * total
                    yield x, z, here[x][z], total

        def over_rows(self, work):
            size = min(8 * GROUP, self.cy) if self.scale == 1.0 else self.cy
            if size == self.cy:
                for row in range(0, size, 8):
                    work(row)
                return

            def body(step, carry):
                for k in range(0, size, 8):
                    work(pl.multiple_of(step * size, 8) + k)
                return carry

            lax.fori_loop(0, self.cy // size, body, 0)

        def start(self, ref):
            def work(row):
                for x in range(self.low):
                    for z in range(self.cz):
                        self.store(ref, x, z, row, self.weight[x] * self.right_side(x, z, row))

            self.over_rows(work)

        def sweep(self, source, target=None, emit=None):
            def work(row):
                for x, z, here, total in self.sums(source, row):
                    f = self.right_side(x, z, row)
                    value = (1.0 - DAMPING) * here + self.weight[x] * (f + total)
                    if emit is None:
                        self.store(target, x, z, row, value)
                    else:
                        emit(x, z, row, value)

            self.over_rows(work)

        def residual(self, ref, spread, coarse_f):
            def work(row):
                parts = {}
                for x, z, here, total in self.sums(ref, row):
                    f = self.right_side(x, z, row)
                    value = f - (self.diag[x] * here - total)
                    key = (x // 2, z // 2)
                    parts[key] = parts[key] + value if key in parts else value
                for (x, z), value in parts.items():
                    spread[pl.ds((x * (self.cz // 2) + z) * self.cy + row, 8), :] = value

            self.over_rows(work)
            for k in range(max(self.low // 2, 1) * self.cz // 2):
                for row in range(0, self.cy // 2, 8):
                    start = k * self.cy + 2 * row
                    coarse_f[pl.ds(k * (self.cy // 2) + row, 8), :] = 0.125 * (
                        spread[pl.ds(start, 8, stride=2), :]
                        + spread[pl.ds(start + 1, 8, stride=2), :]
                    )

        def correct(self, ref, spread, coarse, coarse_ref):
            for x in range(coarse.low):
                for z in range(coarse.cz):
                    for row in range(0, coarse.cy, 8):
                        value = coarse.load(coarse_ref, x, z, row)
                        start = (x * coarse.cz + z) * self.cy + 2 * row
                        spread[pl.ds(start, 8, stride=2), :] = value
                        spread[pl.ds(start + 1, 8, stride=2), :] = value

            def work(row):
                for x in range(self.low):
                    for z in range(self.cz):
                        k = (x * coarse.low // self.low) * coarse.cz + z // 2
                        value = spread[pl.ds(k * self.cy + row, 8), :]
                        self.store(ref, x, z, row, self.load(ref, x, z, row) + value)

            self.over_rows(work)

    def fine_rows(x, z, row):
        return (x // 2) * TILES + z // 2, pl.ds((x % 2) * LANES + (z % 2) * CY + row, 8)

    def fine_f(x, z, row):
        peer, rows = fine_rows(x, z, row)
        return f_ref[peer, rows, :]

    def emit(x, z, row, value):
        peer, rows = fine_rows(x, z, row)
        out_ref[peer, rows, :] = value

    def coarse_f(ref, cz, cy):
        return lambda x, z, row: ref[pl.ds((x * cz + z) * cy + row, 8), :]

    fine = Level(0, va, vb, fine_f, LOW, CZ, CY)
    middle = Level(1, v1a, v1b, coarse_f(f1_ref, CZ // 2, CY // 2), LOW // 2, CZ // 2, CY // 2)
    coarse = Level(2, v2a, v2b, coarse_f(f2_ref, CZ // 4, CY // 4), 1, CZ // 4, CY // 4)

    def coarsest(target):
        cz, cy = coarse.cz, coarse.cy
        tiles = cy // 8
        keys = [(z, r) for z in range(cz) for r in range(tiles)]
        step = LANES // SIDE
        turn = lambda value, j: pltpu.roll(value, j * step, 1) if j else value
        weight = [turn(coarse.weight[0], j) for j in range(SIDE)]
        first = [(high - j) % SIDE == 0 for j in range(SIDE)]
        last = [(high - j) % SIDE == SIDE - 1 for j in range(SIDE)]
        value, right_side = {}, {}
        for z, r in keys:
            f = coarse.right_side(0, z, 8 * r)
            for j in range(SIDE):
                right_side[j, z, r] = weight[j] * turn(f, j)
                value[j, z, r] = right_side[j, z, r]
        row = lax.broadcasted_iota(jnp.int32, shape, 0)
        for left_over in (4, 3, 2, 1, 0):
            new = {}
            for j in range(SIDE):
                if min(j, SIDE - j) > left_over:
                    continue
                for z in range(cz):
                    ups = [pltpu.roll(value[j, z, r], 1, 0) for r in range(tiles)]
                    downs = [pltpu.roll(value[j, z, r], 7, 0) for r in range(tiles)]
                    for r in range(tiles):
                        above = ups[r - 1] if r else zero
                        below = downs[r + 1] if r < tiles - 1 else zero
                        total = jnp.where(row == 0, above, ups[r])
                        total = total + jnp.where(row == 7, below, downs[r])
                        if z > 0:
                            total = total + value[j, z - 1, r]
                        if z < cz - 1:
                            total = total + value[j, z + 1, r]
                        total = total + jnp.where(first[j], zero, value[(j + 1) % SIDE, z, r])
                        total = total + jnp.where(last[j], zero, value[(j - 1) % SIDE, z, r])
                        new[j, z, r] = (
                            (1.0 - DAMPING) * value[j, z, r]
                            + right_side[j, z, r]
                            + (coarse.scale * weight[j]) * total
                        )
            value = new
        for z, r in keys:
            coarse.store(target, 0, z, 8 * r, value[0, z, r])

    for cycle in range(CYCLES):
        if cycle == 0:
            fine.start(vb)
            fine.sweep(vb, va)
        else:
            fine.sweep(va, vb)
            fine.sweep(vb, va)
        fine.residual(va, spread_ref, f1_ref)
        middle.start(v1b)
        middle.sweep(v1b, v1a)
        middle.residual(v1a, spread1_ref, f2_ref)
        coarsest(v2b)
        middle.correct(v1a, spread1_ref, coarse, v2b)
        middle.sweep(v1a, v1b)
        middle.sweep(v1b, v1a)
        fine.correct(va, spread_ref, middle, v1a)
        fine.sweep(va, vb)
        if cycle == CYCLES - 1:
            fine.sweep(vb, emit=emit)
        else:
            fine.sweep(vb, va)


def vmem(count):
    return [pl.BlockSpec(memory_space=pltpu.VMEM)] * count


def rows(count):
    return pltpu.VMEM((count, LANES), jnp.float32)


def exchange(value):
    return lax.all_to_all(value, "ta", split_axis=0, concat_axis=0, tiled=True)


def swaps(start, count):
    pairs = [(i, i + 1) for i in range(start, count - 1, 2)]
    return pairs + [(b, a) for a, b in pairs]


def call(kernel, shape, count, *scratch, smem=0, flops=10**6, out=pltpu.VMEM):
    return pl.pallas_call(
        kernel,
        out_shape=shape,
        in_specs=[pl.BlockSpec(memory_space=pltpu.SMEM)] * smem + vmem(count),
        out_specs=pl.BlockSpec(memory_space=out),
        scratch_shapes=scratch,
        compiler_params=pltpu.CompilerParams(vmem_limit_bytes=LIMIT),
        cost_estimate=pl.CostEstimate(flops=flops, bytes_accessed=2**20, transcendentals=0),
    )


def iteration(source, previous, time_modes, time_back, step_code):
    steps, planes, _ = source.shape
    count = lax.axis_size("gx")
    first, last = previous[:, 0, :], previous[:, planes - 1, :]
    odd = lax.axis_index("gx") % 2 == 1
    outer = lax.ppermute(jnp.where(odd, last, first), "gx", swaps(1, count))
    outer, inner = lax.optimization_barrier((outer, jnp.where(odd, first, last)))
    inner = lax.ppermute(inner, "gx", swaps(0, count))
    by_step = jax.ShapeDtypeStruct((SIDE, planes // 2, steps, LANES), jnp.float32)
    by_mode = jax.ShapeDtypeStruct((SIDE, 2 * LANES, LANES), jnp.float32)
    turned = (TILES * planes * steps, LANES)
    blocks = pltpu.VMEM((SIDE, 2 * LANES, LANES), jnp.float32)

    held = call(turn_kernel, jax.ShapeDtypeStruct(turned, jnp.float32), 3, flops=10**8)(
        source, first, last
    )
    packed = call(pack_kernel, by_step, 3, rows(8))(held, outer, inner)
    mixed = call(forward_kernel, by_mode, 2, blocks)(time_modes, exchange(packed))
    solved = call(
        solver_kernel,
        by_mode,
        1,
        *[rows(8 + LOW * CZ * (CY + 8))] * 2,
        rows(LOW * CZ // 4 * CY),
        rows(LOW * CZ // 4 * CY // 2),
        *[rows(8 + LOW * CZ // 4 * (CY // 2 + 8))] * 2,
        rows(CZ // 4 * CY // 2),
        rows(CZ // 4 * CY // 4),
        *[rows(8 + CZ // 4 * (CY // 4 + 8))] * 2,
        smem=1,
    )(step_code, exchange(mixed))
    mixed = call(backward_kernel, by_step, 2, blocks)(time_back, exchange(solved))
    result = jax.ShapeDtypeStruct(source.shape, jnp.float32)
    stage = pltpu.VMEM((TILES, steps, planes, LANES), jnp.float32)
    sems = pltpu.SemaphoreType.DMA((TILES,))
    return call(unpack_kernel, result, 1, rows(turned[0]), stage, sems, out=pl.ANY)(exchange(mixed))


def solution(mesh):
    placed = (P("ta", "gx", None), P("ta", "gx", None), P(), P(), P("ta"))
    return jax.shard_map(
        iteration, mesh=mesh, in_specs=placed, out_specs=P("ta", "gx", None), check_vma=False
    )
```
